32 devices in a mesh: blk: 32 (over z, y, x, core).
Axes of the slice: x: 2, y: 2, z: 4, core: 2. Of those that a mesh axis runs over, the one named last changes fastest.
Arguments:
- node_latent: bfloat16 [131072, 128], P('blk'), may hold values from -16 to 16
- edge_latent: bfloat16 [786432, 128], P('blk'), may hold values from -6 to 6
- edge_ends: int32 [2, 786432], P(None, 'blk'), may hold values from 0 to 5631, as said below
- edge_owned: int32 [786432], P('blk'), may hold values from 0 to 1, as said below
- send_index: int32 [32, 6, 256], P('blk'), may hold values from 0 to 4095, as said below
- edge_w1: bfloat16 [2, 384, 128], replicated, may hold values from -0.3125 to 0.3125
- edge_b1: float32 [2, 128], replicated, may hold values from -3 to 3
- edge_w2: bfloat16 [2, 128, 128], replicated, may hold values from -0.5 to 0.5
- edge_gain: float32 [2, 128], replicated, may hold values from 0.5 to 1.5
- edge_shift: float32 [2, 128], replicated, may hold values from -2 to 2
- node_w1: bfloat16 [2, 256, 128], replicated, may hold values from -0.375 to 0.375
- node_b1: float32 [2, 128], replicated, may hold values from -3 to 3
- node_w2: bfloat16 [2, 128, 128], replicated, may hold values from -0.5 to 0.5
- node_gain: float32 [2, 128], replicated, may hold values from 0.5 to 1.5
- node_shift: float32 [2, 128], replicated, may hold values from -2 to 2
Outputs:
- node_out: bfloat16 [131072, 128], P('blk')
- edge_out: bfloat16 [786432, 128], P('blk')
The draws below stay inside these ranges and needn't reach their ends.
Inputs may be any that keep to these rules, and one draw needn't show every extreme that they name: edge_ends[0] holds each slot's sender, edge_ends[1] its receiver, as entries of the block's extended node list. Slot s of a block lies in tile t = s // 128; each of its ends is either an own node from (t // 6) * 128 to (t // 6 + 1) * 128 - 1 or a halo entry from 4096 + (t % 6) * 256 to 4096 + (t % 6 + 1) * 256 - 1; at most one end of a slot is a halo entry. `edge_owned`: in each block the slots with 1 come first; every block has at least 15360 of them. send_index[b, k] lists 256 distinct nodes of block b.
All inputs are finite; a program needn't handle non-finite values.
Results may differ from the reference program's by a relative error of at most 0.0085.
Values may be sent and summed in bfloat16 or wider, within the bound.
A program may use at most 128 MiB of HBM per device.

```python
import jax
import jax.numpy as jnp
from jax import lax

LATENT = 128
NODE_DEV = 4096
HALO = 256
LAYERS = 2
FACES = 6
GX = 4
GY = 4
EDGE_TILE = 128
EDGE_DEV = 24576
EDGES = 786432
N_BLK = 32


def draw_node_latent(key, part):
    total_rows = NODE_DEV * N_BLK
    position = jnp.arange(total_rows, dtype=jnp.float32)[:, None] / (total_rows - 1)
    values = jnp.clip(jax.random.normal(key, (total_rows, LATENT), jnp.float32), -5.0, 5.0)
    scales = 1.0 + 2.0 * position
    return (values * scales).astype(jnp.bfloat16)


def draw_edge_ends(key, part):
    total_slots = EDGE_DEV * N_BLK
    subkeys = jax.random.split(jax.random.fold_in(key, 11), 4)
    slot = jnp.arange(total_slots, dtype=jnp.int32) % EDGE_DEV
    tile_id = slot // EDGE_TILE
    own_base = tile_id // FACES * EDGE_TILE
    halo_base = NODE_DEV + tile_id % FACES * HALO
    categories = jax.random.randint(subkeys[0], (total_slots,), 0, 8)
    first_local = jax.random.randint(subkeys[1], (total_slots,), 0, EDGE_TILE)
    step_by = jax.random.randint(subkeys[2], (total_slots,), 1, EDGE_TILE)
    second_local = (first_local + step_by) % EDGE_TILE
    remote = halo_base + jax.random.randint(subkeys[3], (total_slots,), 0, HALO)
    senders = jnp.where(categories < 2, remote, own_base + first_local)
    receivers = jnp.where((categories >= 2) & (categories < 4), remote, own_base + second_local)
    return jnp.stack([senders, receivers]).astype(jnp.int32)


def draw_edge_owned(key, part):
    subkeys = jax.random.split(jax.random.fold_in(key, 17), 2)
    counts = jax.random.randint(subkeys[0], (N_BLK,), EDGE_DEV * 5 // 8, EDGE_DEV + 1)
    fullest = jax.random.randint(subkeys[1], (), 0, N_BLK)
    counts = jnp.where(jnp.arange(N_BLK) == fullest, EDGE_DEV, counts)
    slots = jnp.arange(EDGE_DEV)[None, :] < counts[:, None]
    return slots.astype(jnp.int32).reshape(-1)


def pick_rows(subkey):
    return jax.random.permutation(subkey, NODE_DEV)[:HALO]


def draw_send_index(key, part):
    subkeys = jax.random.split(jax.random.fold_in(key, 23), N_BLK * FACES)
    picked = jax.vmap(pick_rows)(subkeys)
    return picked.reshape(N_BLK, FACES, HALO).astype(jnp.int32)


def steps_of(rng, extent, cuts, least, high):
    loudness, own = 1.0, jax.random.fold_in(rng, 6)
    for dim, parts in cuts:
        steps = jnp.exp(jax.random.uniform(jax.random.fold_in(own, dim), (parts,), jnp.float32, least / len(cuts), high / len(cuts)))
        loudness = loudness * jnp.repeat(steps, extent[dim] // parts).reshape([-1 if axis == dim else 1 for axis in range(len(extent))])
    return loudness


def noise(key, shape, scale, limit, cuts=(), kind=jnp.bfloat16):
    level = steps_of(key, shape, cuts, -0.22, 0.18) if cuts else 1.0
    values = jax.random.normal(key, shape, jnp.float32) * scale * level
    return jnp.minimum(jnp.maximum(values, -limit), limit).astype(kind)


def setup_inputs(seed: int = 0) -> dict:
    arg_keys = jax.random.split(jax.random.key(seed), 16)
    node_latent = draw_node_latent(jax.random.fold_in(arg_keys[15], 71), 0)
    edge_latent = noise(arg_keys[1], (EDGES, LATENT), 1.0, 6.0, ((0, 32),))
    edge_ends = draw_edge_ends(jax.random.fold_in(arg_keys[15], 71), 0)
    edge_owned = draw_edge_owned(jax.random.fold_in(arg_keys[15], 71), 0)
    send_index = draw_send_index(jax.random.fold_in(arg_keys[15], 71), 0)
    edge_w1 = noise(arg_keys[5], (LAYERS, 3 * LATENT, LATENT), (3 * LATENT) ** -0.5, 0.3125)
    edge_b1 = noise(arg_keys[6], (LAYERS, LATENT), 0.5, 3.0, (), jnp.float32)
    edge_w2 = noise(arg_keys[7], (LAYERS, LATENT, LATENT), LATENT ** -0.5, 0.5)
    edge_gain = jnp.clip(1.0 + 0.1 * jax.random.normal(arg_keys[8], (LAYERS, LATENT), jnp.float32), 0.5, 1.5)
    edge_shift = noise(arg_keys[9], (LAYERS, LATENT), 0.3, 2.0, (), jnp.float32)
    node_w1 = noise(arg_keys[10], (LAYERS, 2 * LATENT, LATENT), (2 * LATENT) ** -0.5, 0.375)
    node_b1 = noise(arg_keys[11], (LAYERS, LATENT), 0.5, 3.0, (), jnp.float32)
    node_w2 = noise(arg_keys[12], (LAYERS, LATENT, LATENT), LATENT ** -0.5, 0.5)
    node_gain = jnp.clip(1.0 + 0.1 * jax.random.normal(arg_keys[13], (LAYERS, LATENT), jnp.float32), 0.5, 1.5)
    node_shift = noise(arg_keys[14], (LAYERS, LATENT), 0.3, 2.0, (), jnp.float32)
    return {"node_latent": node_latent, "edge_latent": edge_latent, "edge_ends": edge_ends, "edge_owned": edge_owned, "send_index": send_index, "edge_w1": edge_w1, "edge_b1": edge_b1, "edge_w2": edge_w2, "edge_gain": edge_gain, "edge_shift": edge_shift, "node_w1": node_w1, "node_b1": node_b1, "node_w2": node_w2, "node_gain": node_gain, "node_shift": node_shift}


def row_norm(mixed):
    centre = mixed - lax.optimization_barrier(jnp.mean(mixed, axis=1, keepdims=True))
    spread = lax.optimization_barrier(jnp.mean(centre * centre, axis=1, keepdims=True))
    return centre * lax.rsqrt(spread + 1e-05)

def reference(node_latent, edge_latent, edge_ends, edge_owned, send_index, edge_w1, edge_b1, edge_w2, edge_gain, edge_shift, node_w1, node_b1, node_w2, node_gain, node_shift):
    offsets = jnp.array([1, -1, GX, -GX, GX * GY, -GX * GY], dtype=jnp.int32)
    blocks = jnp.arange(N_BLK, dtype=jnp.int32)
    source = jnp.mod(blocks[:, None] - offsets[None, :], N_BLK).astype(jnp.int32)
    face_ids = jnp.arange(FACES, dtype=jnp.int32)[None, :]
    halo_nodes = source[:, :, None] * NODE_DEV + send_index[source, face_ids]
    own_nodes = blocks[:, None] * NODE_DEV + jnp.arange(NODE_DEV, dtype=jnp.int32)[None, :]
    lookup = jnp.concatenate([own_nodes, halo_nodes.reshape(N_BLK, FACES * HALO)], axis=1).astype(jnp.int32)
    ends = edge_ends.reshape(2, N_BLK, EDGE_DEV)
    senders = jnp.take_along_axis(lookup, ends[0], axis=1)
    receivers = jnp.take_along_axis(lookup, ends[1], axis=1)
    owned = edge_owned.reshape(N_BLK, EDGE_DEV).astype(jnp.float32)
    latents = node_latent
    edge_state = edge_latent.reshape(N_BLK, EDGE_DEV, LATENT)
    for layer_id in range(LAYERS):

        def edge_block(totals, item, latents=latents, layer_id=layer_id):
            block_edges, block_send, block_recv, block_owned = item
            joined = jnp.concatenate([block_edges, latents[block_send], latents[block_recv]], axis=1)
            hidden = jax.nn.relu(jnp.dot(joined, edge_w1[layer_id], preferred_element_type=jnp.float32) + edge_b1[layer_id]).astype(jnp.bfloat16)
            mixed = jnp.dot(hidden, edge_w2[layer_id], preferred_element_type=jnp.float32)
            normed = edge_gain[layer_id] * row_norm(mixed) + edge_shift[layer_id]
            edges_new = (block_edges.astype(jnp.float32) + block_owned[:, None] * normed).astype(jnp.bfloat16)
            totals = totals.at[block_recv].add(block_owned[:, None] * edges_new.astype(jnp.float32))
            return (totals, edges_new)
        start = jnp.zeros((N_BLK * NODE_DEV, LATENT), jnp.float32)
        totals, edge_state = lax.scan(edge_block, start, (edge_state, senders, receivers, owned))
        aggregate = totals.astype(jnp.bfloat16)
        node_in = jnp.concatenate([latents, aggregate], axis=1)
        node_hidden = jax.nn.relu(jnp.dot(node_in, node_w1[layer_id], preferred_element_type=jnp.float32) + node_b1[layer_id]).astype(jnp.bfloat16)
        update = jnp.dot(node_hidden, node_w2[layer_id], preferred_element_type=jnp.float32)
        centre_mean = lax.optimization_barrier(jnp.mean(update, axis=0))
        deviation = update - centre_mean
        variance = lax.optimization_barrier(jnp.mean(deviation * deviation, axis=0))
        latents = (latents.astype(jnp.float32) + node_gain[layer_id] * deviation * lax.rsqrt(variance + 1e-05) + node_shift[layer_id]).astype(jnp.bfloat16)
    return (latents, edge_state.reshape(N_BLK * EDGE_DEV, LATENT))
```

```python
import functools

import jax
import jax.numpy as jnp
from jax import lax
from jax.experimental import pallas as pl
from jax.experimental.pallas import tpu as pltpu
from jax.sharding import PartitionSpec as P

LAYERS = 2
FACES = 6
GX = 4
GY = 4
MESH = pl.DeviceIdType.MESH
VMEM = pltpu.VMEM
F32 = jnp.float32
BF16 = jnp.bfloat16


def dot(a, b):
    return jnp.dot(a, b, preferred_element_type=F32)


def hot(mask):
    return jnp.where(mask, 1.0, 0.0).astype(BF16)


def iota(shape, axis):
    return lax.broadcasted_iota(jnp.int32, shape, axis)


def face_target(me, face, n, sign):
    step = jnp.where(face < 2, 1, jnp.where(face < 4, GX, GX * GY))
    step = jnp.where(face % 2 == 0, step, -step) * sign
    return lax.rem(me + step + n * GX * GY, n)


def edge_kernel(layer, own_rows, halo_rows, e_ref, ends_ref, owned_ref, tab_ref, phalo_ref,
                w1_ref, b1_ref, w2_ref, gain_ref, shift_ref,
                out_ref, own_ref, halo_ref, acc, bd1, bd2):
    step = pl.program_id(0)
    steps = pl.num_programs(0)
    tile = ends_ref.shape[3]
    width = e_ref.shape[1]
    rows = FACES * tile

    @pl.when(step == 0)
    def _():
        acc[...] = jnp.zeros_like(acc)
        bd1[...] = jnp.zeros_like(bd1)
        bd2[...] = jnp.zeros_like(bd2)
        for i in range(2):
            bd1[i * width:(i + 1) * width, i * width:(i + 1) * width] = w1_ref[layer, 0:width, :]
            bd2[i * width:(i + 1) * width, i * width:(i + 1) * width] = w2_ref[layer]

    per_step = ends_ref.shape[1]
    face = iota((FACES, tile), 0)
    lane = iota((rows, tile), 1)
    bias = b1_ref[layer:layer + 1, :]
    gain = gain_ref[layer:layer + 1, :]
    shift = shift_ref[layer:layer + 1, :]
    for pair in range(per_step // 2):
        hots, tables, recv_rows, halo_recv, flags_r, flags_o, pre = [], [], [], [], [], [], []
        halo_hots = []
        for i in range(2):
            local = pair * 2 + i
            group = step * per_step + local
            s = ends_ref[0, local]
            r = ends_ref[1, local]
            ok = owned_ref[local] > 0
            s_halo = s >= own_rows
            r_halo = r >= own_rows
            so = jnp.where(ok & ~s_halo, s - group * tile, 255)
            ro = jnp.where(ok & ~r_halo, r - group * tile, 255)
            base = own_rows + face * halo_rows
            hs = jnp.where(s_halo, s - base, jnp.where(r_halo, r - base, 511))
            hc = jnp.where(ok, hs, 511)
            recv_rows.append(ro)
            halo_recv.append(jnp.where(ok & r_halo, r - base, 511))
            code = (so | (ro << 8) | (hc << 16) | jnp.where(r_halo, 1 << 25, 0)
                    | jnp.where(ok, 1 << 26, 0))
            cols = jnp.concatenate(
                [jnp.broadcast_to(code[k:k + 1, :], (tile, tile)).T for k in range(FACES)], axis=0)
            sr = jnp.concatenate(
                [hot((cols & 255) == lane), hot(((cols >> 8) & 255) == lane)], axis=1)
            hcol = (cols >> 16) & 511
            halo_hots.append(jnp.concatenate([hot(hcol == lane + j * tile)
                                              for j in range(halo_rows // tile)], axis=1))
            flags_r.append((cols & (1 << 25)) != 0)
            flags_o.append((cols & (1 << 26)) != 0)
            pre.append(dot(sr, tab_ref[local]))
        from_halo = [[], []]
        for k in range(FACES):
            at = slice(k * tile, (k + 1) * tile)
            both = dot(jnp.concatenate([halo_hots[0][at], halo_hots[1][at]], axis=0), phalo_ref[k])
            for i in range(2):
                part = both[i * tile:(i + 1) * tile]
                from_halo[i].append(jnp.where(flags_r[i][at], part[:, width:], part[:, :width]))
        edges = [e_ref[(pair * 2 + i) * rows:(pair * 2 + i + 1) * rows, :] for i in range(2)]
        from_e = dot(jnp.concatenate(edges, axis=1), bd1[...])
        hidden = []
        for i in range(2):
            before = from_e[:, i * width:(i + 1) * width] + pre[i] + jnp.concatenate(from_halo[i], axis=0)
            hidden.append(jnp.maximum(before + bias, 0.0).astype(BF16))
        mixed2 = dot(jnp.concatenate(hidden, axis=1), bd2[...])
        fresh = []
        for i in range(2):
            mixed = mixed2[:, i * width:(i + 1) * width]
            centre = mixed - jnp.mean(mixed, axis=1, keepdims=True)
            spread = jnp.mean(centre * centre, axis=1, keepdims=True)
            normed = gain * (centre * lax.rsqrt(spread + 1e-05)) + shift
            new = (edges[i].astype(F32) + jnp.where(flags_o[i], normed, 0.0)).astype(BF16)
            out_ref[(pair * 2 + i) * rows:(pair * 2 + i + 1) * rows, :] = new
            fresh.append(new)
            node = iota((tile, tile), 0)
            hot_t = jnp.concatenate([hot(recv_rows[i][k:k + 1, :] == node) for k in range(FACES)], axis=1)
            own_ref[(pair * 2 + i) * tile:(pair * 2 + i + 1) * tile, :] = dot(hot_t, new)
        node = iota((halo_rows, tile), 0)
        for k in range(FACES):
            at = slice(k * tile, (k + 1) * tile)
            hot_t = jnp.concatenate([hot(halo_recv[i][k:k + 1, :] == node) for i in range(2)], axis=1)
            acc[k] += dot(hot_t, jnp.concatenate([fresh[0][at], fresh[1][at]], axis=0))

    @pl.when(step == steps - 1)
    def _():
        halo_ref[...] = acc[...].astype(BF16)


def edge_layer(layer, e, ends, owned, tab, phalo, w1, b1, w2, gain, shift, own_rows, halo_rows):
    groups, tile = ends.shape[1], ends.shape[3]
    width = e.shape[1]
    per = 4 if groups % 4 == 0 else 2
    rows = FACES * tile
    whole = lambda a: pl.BlockSpec(a.shape, lambda i: (0,) * a.ndim)
    return pl.pallas_call(
        functools.partial(edge_kernel, layer, own_rows, halo_rows),
        grid=(groups // per,),
        in_specs=[
            pl.BlockSpec((per * rows, width), lambda i: (i, 0)),
            pl.BlockSpec((2, per, FACES, tile), lambda i: (0, i, 0, 0)),
            pl.BlockSpec((per, FACES, tile), lambda i: (i, 0, 0)),
            pl.BlockSpec((per, 2 * tile, width), lambda i: (i, 0, 0)),
            whole(phalo), whole(w1), whole(b1), whole(w2), whole(gain), whole(shift),
        ],
        out_specs=[
            pl.BlockSpec((per * rows, width), lambda i: (i, 0)),
            pl.BlockSpec((per * tile, width), lambda i: (i, 0)),
            pl.BlockSpec((FACES, halo_rows, width), lambda i: (0, 0, 0)),
        ],
        out_shape=[
            jax.ShapeDtypeStruct(e.shape, BF16),
            jax.ShapeDtypeStruct((own_rows, width), F32),
            jax.ShapeDtypeStruct((FACES, halo_rows, width), BF16),
        ],
        scratch_shapes=[
            VMEM((FACES, halo_rows, width), F32),
            VMEM((2 * width, 2 * width), BF16),
            VMEM((2 * width, 2 * width), BF16),
        ],
        compiler_params=pltpu.CompilerParams(dimension_semantics=("arbitrary",)),
    )(e, ends, owned, tab, phalo, w1, b1, w2, gain, shift)


def first_weights(w1_ref, layer, width):
    return jnp.concatenate(
        [w1_ref[layer, width:2 * width, :], w1_ref[layer, 2 * width:3 * width, :]], axis=1)


def exchange_latents(me, n, layer, h_ref, send_ref, w1_ref, tab_ref, phalo_ref, stage, landed, ssem, rsem):
    own_rows, width = h_ref.shape
    halo_rows = send_ref.shape[1]
    tile = 128
    chunk = min(1024, own_rows)
    weights = first_weights(w1_ref, layer, width)

    def copy(k):
        return pltpu.make_async_remote_copy(
            src_ref=stage.at[k], dst_ref=landed.at[k], send_sem=ssem.at[k], recv_sem=rsem.at[k],
            device_id=(face_target(me, k, n, 1),), device_id_type=MESH)

    @pl.loop(0, FACES)
    def _(k):
        row = send_ref[pl.ds(k, 1), :]
        cols = jnp.concatenate(
            [jnp.broadcast_to(row[:, j * tile:(j + 1) * tile], (tile, tile)).T
             for j in range(halo_rows // tile)], axis=0)
        lane = iota(cols.shape, 1)
        total = None
        for c in range(own_rows // chunk):
            one = jnp.concatenate(
                [hot(cols == lane + (c * chunk + j * tile)) for j in range(chunk // tile)], axis=1)
            part = dot(one, h_ref[c * chunk:(c + 1) * chunk, :])
            total = part if total is None else total + part
        stage[pl.ds(k, 1)] = total.astype(BF16)[None]
        copy(k).start()

    @pl.loop(0, tab_ref.shape[0])
    def _(g):
        both = dot(h_ref[pl.ds(pl.multiple_of(g * tile, tile), tile), :], weights).astype(BF16)
        tab_ref[pl.ds(g, 1)] = jnp.concatenate([both[:, :width], both[:, width:]], axis=0)[None]

    @pl.loop(0, FACES)
    def _(k):
        copy(k).wait()
        phalo_ref[pl.ds(k, 1)] = dot(landed[k], weights).astype(BF16)[None]


def first_kernel(n, h_ref, send_ref, w1_ref, tab_ref, phalo_ref, stage, landed, ssem, rsem):
    me = lax.axis_index("blk")
    barrier = pltpu.get_barrier_semaphore()
    for k in range(FACES):
        pl.semaphore_signal(barrier, inc=1, device_id=(face_target(me, k, n, 1),), device_id_type=MESH)
    pl.semaphore_wait(barrier, FACES)
    exchange_latents(me, n, 0, h_ref, send_ref, w1_ref, tab_ref, phalo_ref, stage, landed, ssem, rsem)


def node_kernel(n, layer, last, h_ref, own_ref, halo_ref, send_ref, ew1_ref, w1_ref, b1_ref, w2_ref,
                gain_ref, shift_ref, *rest):
    if last:
        out_ref, returned, update, mine, stats, ssem, rsem, tsem, usem = rest
    else:
        (out_ref, tab_ref, phalo_ref, returned, update, mine, stats, ssem, rsem, tsem, usem,
         stage, landed, ssem2, rsem2) = rest
    me = lax.axis_index("blk")
    own_rows, width = h_ref.shape
    halo_rows = send_ref.shape[1]
    barrier = pltpu.get_barrier_semaphore()

    @pl.loop(1, n)
    def _(j):
        pl.semaphore_signal(barrier, inc=1, device_id=(lax.rem(me + j, n),), device_id_type=MESH)

    pl.semaphore_wait(barrier, n - 1)

    def copy(k):
        return pltpu.make_async_remote_copy(
            src_ref=halo_ref.at[k], dst_ref=returned.at[k], send_sem=ssem.at[k], recv_sem=rsem.at[k],
            device_id=(face_target(me, k, n, -1),), device_id_type=MESH)

    for k in range(FACES):
        copy(k).start()
    for k in range(FACES):
        copy(k).wait()
    back = returned[...].reshape(FACES * halo_rows, width)
    chunk = min(512, own_rows)

    def body(c, carry):
        sums, squares = carry
        first = pl.multiple_of(c * chunk, chunk)
        at = pl.ds(first, chunk)
        node = iota((chunk, halo_rows), 0) + first
        one = jnp.concatenate([hot(send_ref[k:k + 1, :] == node) for k in range(FACES)], axis=1)
        agg = (own_ref[at, :] + dot(one, back)).astype(BF16)
        joined = jnp.concatenate([h_ref[at, :], agg], axis=1)
        hidden = jnp.maximum(dot(joined, w1_ref[layer]) + b1_ref[layer:layer + 1, :], 0.0).astype(BF16)
        upd = dot(hidden, w2_ref[layer])
        update[at, :] = upd
        return (sums + jnp.sum(upd, axis=0, keepdims=True),
                squares + jnp.sum(upd * upd, axis=0, keepdims=True))

    zero = jnp.zeros((1, width), F32)
    sums, squares = lax.fori_loop(0, own_rows // chunk, body, (zero, zero))
    packed = jnp.concatenate([sums, squares, jnp.zeros((6, width), F32)], axis=0)
    mine[...] = packed
    stats[pl.ds(me, 1)] = packed[None]

    def share(j):
        return pltpu.make_async_remote_copy(
            src_ref=mine, dst_ref=stats.at[me], send_sem=tsem.at[j], recv_sem=usem.at[j],
            device_id=(lax.rem(me + j, n),), device_id_type=MESH)

    @pl.loop(1, n)
    def _(j):
        share(j).start()

    @pl.loop(1, n)
    def _(j):
        share(j).wait()

    total = jnp.sum(stats[...], axis=0)
    count = own_rows * n
    mean = total[0:1] / count
    variance = jnp.maximum(total[1:2] / count - mean * mean, 0.0)
    scale = gain_ref[layer:layer + 1, :] * lax.rsqrt(variance + 1e-05)
    shift = shift_ref[layer:layer + 1, :]

    @pl.loop(0, own_rows // chunk)
    def _(c):
        at = pl.ds(pl.multiple_of(c * chunk, chunk), chunk)
        out_ref[at, :] = (h_ref[at, :].astype(F32) + scale * (update[at, :] - mean) + shift).astype(BF16)

    if not last:
        exchange_latents(me, n, layer + 1, out_ref, send_ref, ew1_ref, tab_ref, phalo_ref,
                         stage, landed, ssem2, rsem2)


def per_device(n, node_latent, edge_latent, edge_ends, edge_owned, send_index, edge_w1, edge_b1, edge_w2,
               edge_gain, edge_shift, node_w1, node_b1, node_w2, node_gain, node_shift):
    own_rows, width = node_latent.shape
    halo_rows = send_index.shape[2]
    tile = 128
    groups = own_rows // tile
    ends = edge_ends.reshape(2, groups, FACES, tile)
    owned = edge_owned.reshape(groups, FACES, tile)
    send = send_index[0]
    tab_shape = jax.ShapeDtypeStruct((groups, 2 * tile, width), BF16)
    phalo_shape = jax.ShapeDtypeStruct((FACES, halo_rows, 2 * width), BF16)
    spec = pl.BlockSpec(memory_space=VMEM)
    faces = VMEM((FACES, halo_rows, width), BF16)
    sems = pltpu.SemaphoreType.DMA((FACES,))
    tab, phalo = pl.pallas_call(
        functools.partial(first_kernel, n),
        in_specs=[spec] * 3,
        out_specs=[spec] * 2,
        out_shape=[tab_shape, phalo_shape],
        scratch_shapes=[faces, faces, sems, sems],
        compiler_params=pltpu.CompilerParams(collective_id=0, has_side_effects=True),
    )(node_latent, send, edge_w1)
    latents, edges = node_latent, edge_latent
    for layer in range(LAYERS):
        edges, own_sums, halo_sums = edge_layer(
            layer, edges, ends, owned, tab, phalo, edge_w1, edge_b1, edge_w2, edge_gain, edge_shift,
            own_rows, halo_rows)
        last = layer == LAYERS - 1
        out = [jax.ShapeDtypeStruct((own_rows, width), BF16)]
        scratch = [faces, VMEM((own_rows, width), F32), VMEM((8, width), F32), VMEM((n, 8, width), F32),
                   sems, sems, pltpu.SemaphoreType.DMA((n,)), pltpu.SemaphoreType.DMA((n,))]
        if not last:
            out += [tab_shape, phalo_shape]
            scratch += [faces, faces, sems, sems]
        result = pl.pallas_call(
            functools.partial(node_kernel, n, layer, last),
            in_specs=[spec] * 10,
            out_specs=[spec] * len(out),
            out_shape=out,
            scratch_shapes=scratch,
            compiler_params=pltpu.CompilerParams(collective_id=1 + layer, has_side_effects=True),
        )(latents, own_sums, halo_sums, send, edge_w1, node_w1, node_b1, node_w2, node_gain, node_shift)
        latents = result[0]
        if not last:
            tab, phalo = result[1:]
    return (latents, edges)


def solution(mesh):
    row, rep = P("blk", None), P()
    return jax.shard_map(
        functools.partial(per_device, mesh.shape["blk"]),
        mesh=mesh,
        in_specs=(row, row, P(None, "blk"), P("blk"), P("blk", None, None)) + (rep,) * 10,
        out_specs=(row, row),
        check_vma=False,
    )
```
